32 devices in a mesh: row: 8 (over z, x), col: 4 (over y, core).
Axes of the slice: x: 2, y: 2, z: 4, core: 2. Of those that a mesh axis runs over, the one named last changes fastest.
Arguments:
- gradients: bfloat16 [8, 4, 4, 64, 1536], P('row', 'col'), may hold values from -96 to 96
- token_counts: int32 [8, 4], P('row', 'col'), may hold values from 16 to 256
- row_groups: int32 [2, 8, 4], replicated, may hold values from 0 to 3, each once within a row
- col_groups: int32 [1, 4, 8], replicated, may hold values from 0 to 7, each once within a row
Outputs:
- averaged: float32 [8, 4, 4, 64, 1536], P('row', 'col')
- totals: int32 [8, 4], P('row', 'col')
The draws below stay inside these ranges and needn't reach their ends.
Inputs may be any that keep to these rules, and one draw needn't show every extreme that they name: row_groups[r, i] lists the 4 grid columns in some order: in row round r, grid row i's member of group g sits in column row_groups[r, i, g]. col_groups[0, j] lists the 8 grid rows in some order: grid column j's member of group h sits in row col_groups[0, j, h].
All inputs are finite; a program needn't handle non-finite values.
Results may differ from the reference program's by a relative error of at most 0.0003.
Values may be sent and summed in bfloat16 or wider, within the bound.
A program may use at most 64 MiB of HBM per device.

```python
import jax
import jax.numpy as jnp

D = 1536
BLOCKS = 4
GR = 64
N_ROW = 8
N_COL = 4


def with_ends(drawn, rng, smallest, largest):
    spot = [jax.random.randint(jax.random.fold_in(rng, axis), (), 0, length) for axis, length in enumerate(drawn.shape)]
    widest = drawn.shape.index(max(drawn.shape))
    beside = spot[:widest] + [(spot[widest] + 1) % drawn.shape[widest]] + spot[widest + 1:]
    return drawn.at[tuple(spot)].set(smallest).at[tuple(beside)].set(largest)


def block_scale(rng, dims, split, smallest, high):
    def one(dim, blocks):
        steps = jax.random.uniform(jax.random.fold_in(jax.random.fold_in(rng, 6), dim), (blocks,), jnp.float32, smallest / len(split), high / len(split))
        return jnp.repeat(jnp.exp(steps), dims[dim] // blocks).reshape((-1,) + (1,) * (len(dims) - dim - 1))

    level = one(*split[0])
    for cut in split[1:]:
        level = level * one(*cut)
    return level


def centred(rng, extent, deviation, reach, pieces=(), dtype=jnp.bfloat16):
    array = deviation * jax.random.normal(rng, extent, jnp.float32)
    if pieces:
        array = array * block_scale(rng, extent, pieces, -0.22, 0.18)
    return jnp.clip(array, -reach, reach).astype(dtype)


def setup_inputs(seed: int = 0) -> dict:
    seeds = jax.random.split(jax.random.key(seed), 5)
    return {
        "gradients": centred(seeds[0], (N_ROW, N_COL, BLOCKS, GR, D), 16.0, 96.0, ((0, 8), (1, 4))),
        "token_counts": with_ends(jax.random.randint(seeds[1], (N_ROW, N_COL), 16, 257), jax.random.fold_in(seeds[1], 1), 16, 256).astype(jnp.int32),
        "row_groups": jax.vmap(lambda own: jax.random.permutation(own, N_COL))(jax.random.split(seeds[2], 2 * N_ROW)).reshape((2, N_ROW, N_COL)).astype(jnp.int32),
        "col_groups": jax.vmap(lambda own: jax.random.permutation(own, N_ROW))(jax.random.split(seeds[3], 1 * N_COL)).reshape((1, N_COL, N_ROW)).astype(jnp.int32),
    }


def groups_average(values, weights, group_order):
    picked = jnp.take_along_axis(values, group_order[:, :, None, None], axis=1)
    picked_w = jnp.take_along_axis(weights, group_order, axis=1)
    group_sums = jnp.sum(picked * picked_w[:, :, None, None], axis=0)
    group_totals = jnp.sum(picked_w, axis=0)
    averaged = group_sums / group_totals[:, None, None]
    inverse = jnp.argsort(group_order, axis=1).astype(jnp.int32)
    return averaged[inverse], group_totals[inverse]


def reference(gradients, token_counts, row_groups, col_groups):
    grad_state = gradients.reshape(N_ROW, N_COL, BLOCKS * GR, D).astype(jnp.float32)
    weight = token_counts.astype(jnp.float32)
    grad_state, weight = groups_average(grad_state, weight, row_groups[0])
    swapped, swapped_w = groups_average(jnp.swapaxes(grad_state, 0, 1), weight.T, col_groups[0])
    grad_state = jnp.swapaxes(swapped, 0, 1)
    weight = swapped_w.T
    grad_state, weight = groups_average(grad_state, weight, row_groups[1])
    return grad_state.reshape(gradients.shape), weight.astype(jnp.int32)
```

```python
import functools

import jax
import jax.numpy as jnp
from jax import lax
from jax.experimental import pallas as pl
from jax.experimental.pallas import tpu as pltpu
from jax.sharding import PartitionSpec as P

MESH = pl.DeviceIdType.MESH
F32 = jnp.float32
SKEW = 2


def path_counts(row_groups, col_groups):
    rows, cols = row_groups.shape[1], row_groups.shape[2]
    row_ids = jnp.arange(rows, dtype=jnp.int32)
    col_ids = jnp.arange(cols, dtype=jnp.int32)
    first = (row_groups[0][:, None, :] == col_ids[None, :, None]).astype(F32)
    last = (row_groups[1][:, None, :] == col_ids[None, :, None]).astype(F32)
    between = (col_groups[0][None, :, :] == row_ids[:, None, None]).astype(F32)
    exact = functools.partial(jnp.einsum, precision=lax.Precision.HIGHEST)
    to_second = exact("ijh,ijg->hg", between, first)
    to_third = exact("ijk,ijh->kh", last, between)
    paths = exact("kh,hg->kg", to_third, to_second)
    coefficient = exact("ijg,kg->ijk", first, paths)
    groups = jnp.arange(cols, dtype=F32)
    chosen = jnp.sum(last * groups[None, None, :], axis=2).astype(jnp.int32)
    return coefficient.reshape(rows * cols, cols), chosen.reshape(rows * cols)


def kernel(
    geometry,
    coef_ref, chosen_ref, count_ref, x_ref,
    out_ref, total_ref,
    recv, own, up_out, up_in, down_out, down_in, tot, ret,
    cnt_send, cnt, part_send, parts, inverse,
    x_send_sem, x_recv_sem, r_send_sem, r_recv_sem, z_send_sem, z_recv_sem,
    c_send_sem, c_recv_sem, p_send_sem, p_recv_sem,
):
    across, cols, depth, chunks, wide, groups = geometry
    plane = across * cols
    row, col = lax.axis_index("row"), lax.axis_index("col")
    z = row // across
    me = (row % across) * cols + col

    def member(q):
        return (z * across + q // cols, q % cols)

    def level(other):
        return (other * across + row % across, col)

    def lanes(k):
        return pl.ds(pl.multiple_of(k * wide, 128), wide)

    barrier = pltpu.get_barrier_semaphore()
    for d in range(1, plane):
        pl.semaphore_signal(barrier, inc=1, device_id=member((me + d) % plane), device_id_type=MESH)
    for d in range(1, depth):
        pl.semaphore_signal(barrier, inc=1, device_id=level((z + d) % depth), device_id_type=MESH)
    count = count_ref[0, 0].astype(F32)
    cnt_send[...] = jnp.full(cnt_send.shape, count, F32)
    cnt[me] = jnp.full(cnt_send.shape, count, F32)
    pl.semaphore_wait(barrier, plane + depth - 2)

    def count_copy(d):
        to = (me + d) % plane
        return pltpu.make_async_remote_copy(
            src_ref=cnt_send, dst_ref=cnt.at[me], send_sem=c_send_sem.at[to], recv_sem=c_recv_sem.at[me],
            device_id=member(to), device_id_type=MESH)

    def count_arrival(q):
        return pltpu.make_async_remote_copy(
            src_ref=cnt_send, dst_ref=cnt.at[q], send_sem=c_send_sem.at[q], recv_sem=c_recv_sem.at[q],
            device_id=member(q), device_id_type=MESH)

    def part_copy(d):
        to = (z + d) % depth
        return pltpu.make_async_remote_copy(
            src_ref=part_send, dst_ref=parts.at[z], send_sem=p_send_sem.at[to], recv_sem=p_recv_sem.at[z],
            device_id=level(to), device_id_type=MESH)

    def part_arrival(s):
        return pltpu.make_async_remote_copy(
            src_ref=part_send, dst_ref=parts.at[s], send_sem=p_send_sem.at[s], recv_sem=p_recv_sem.at[s],
            device_id=level(s), device_id_type=MESH)

    def piece_copy(k, to, slot):
        return pltpu.make_async_remote_copy(
            src_ref=x_ref.at[to, :, lanes(k)], dst_ref=recv.at[k, slot],
            send_sem=x_send_sem.at[k, to], recv_sem=x_recv_sem.at[k, slot],
            device_id=member(to), device_id_type=MESH)

    def result_copy(k, to, slot):
        return pltpu.make_async_remote_copy(
            src_ref=ret.at[k, to], dst_ref=out_ref.at[slot, :, lanes(k)],
            send_sem=r_send_sem.at[k, to], recv_sem=r_recv_sem.at[k, slot],
            device_id=member(to), device_id_type=MESH)

    def result_local(k):
        return pltpu.make_async_copy(ret.at[k, me], out_ref.at[me, :, lanes(k)], r_recv_sem.at[k, me])

    def up_copy(k):
        return pltpu.make_async_remote_copy(
            src_ref=up_out.at[k], dst_ref=up_in.at[k], send_sem=z_send_sem.at[0, k], recv_sem=z_recv_sem.at[0, k],
            device_id=level((z + 1) % depth), device_id_type=MESH)

    def down_copy(k):
        return pltpu.make_async_remote_copy(
            src_ref=down_out.at[k], dst_ref=down_in.at[k], send_sem=z_send_sem.at[1, k], recv_sem=z_recv_sem.at[1, k],
            device_id=level((z + depth - 1) % depth), device_id_type=MESH)

    @pl.loop(1, plane)
    def _(d):
        count_copy(d).start()

    @pl.loop(0, chunks)
    def _(k):
        @pl.loop(1, plane)
        def _(d):
            piece_copy(k, (me + d) % plane, me).start()

    @pl.when(z == 0)
    def _():
        up_in[...] = jnp.zeros(up_in.shape, F32)

    @pl.when(z == depth - 1)
    def _():
        down_in[...] = jnp.zeros(down_in.shape, F32)

    @pl.loop(1, plane)
    def _(d):
        count_arrival((me + d) % plane).wait_recv()

    def factor(q, g):
        return coef_ref[(z * across) * cols + q, g] * cnt[q]

    for g in range(groups):
        part = factor(0, g)
        for q in range(1, plane):
            part = part + factor(q, g)
        part_send[g] = part
        parts[z, g] = part

    @pl.loop(1, depth)
    def _(d):
        part_copy(d).start()

    far = jnp.maximum(z, depth - 1 - z)

    @pl.loop(0, chunks + SKEW * (depth - 1))
    def _(t):
        @pl.when(t < chunks)
        def _():
            recv[t, me] = x_ref[me, :, lanes(t)]

            @pl.loop(1, plane)
            def _(d):
                piece_copy(t, me, (me + d) % plane).wait_recv()

            sums = [None] * groups
            for q in range(plane):
                piece = recv[t, q].astype(F32)
                for g in range(groups):
                    term = piece * factor(q, g)
                    sums[g] = term if q == 0 else sums[g] + term
            for g in range(groups):
                own[t, g] = sums[g]

        up = t - SKEW * z

        @pl.when((up >= 0) & (up < chunks))
        def _():
            @pl.when(z > 0)
            def _():
                up_copy(up).wait_recv()

            @pl.when(z < depth - 1)
            def _():
                up_out[up] = own[up] + up_in[up]
                up_copy(up).start()

        down = t - SKEW * (depth - 1 - z)

        @pl.when((down >= 0) & (down < chunks))
        def _():
            @pl.when(z < depth - 1)
            def _():
                down_copy(down).wait_recv()

            @pl.when(z > 0)
            def _():
                down_out[down] = own[down] + down_in[down]
                down_copy(down).start()

        end = t - SKEW * far

        @pl.when(end == 0)
        def _():
            @pl.loop(1, depth)
            def _(d):
                part_arrival((z + d) % depth).wait_recv()

            for g in range(groups):
                weight = parts[0, g]
                for s in range(1, depth):
                    weight = weight + parts[s, g]
                parts[z, g] = weight
                inverse[g] = 1.0 / weight
            total_ref[...] = parts[z, chosen_ref[row * cols + col]].astype(jnp.int32)

        @pl.when((end >= 0) & (end < chunks))
        def _():
            for g in range(groups):
                tot[g] = (own[end, g] + up_in[end, g] + down_in[end, g]) * inverse[g]

            @pl.loop(1, plane)
            def _(d):
                to = (me + d) % plane
                ret[end, to] = tot[chosen_ref[(z * across) * cols + to]]
                result_copy(end, to, me).start()

            ret[end, me] = tot[chosen_ref[row * cols + col]]
            result_local(end).start()

    @pl.loop(1, plane)
    def _(d):
        count_copy(d).wait_send()

    @pl.loop(1, depth)
    def _(d):
        part_copy(d).wait_send()

    @pl.loop(0, chunks)
    def _(k):
        @pl.when(z < depth - 1)
        def _():
            up_copy(k).wait_send()

        @pl.when(z > 0)
        def _():
            down_copy(k).wait_send()

        @pl.loop(1, plane)
        def _(d):
            piece_copy(k, (me + d) % plane, me).wait_send()
            result_copy(k, (me + d) % plane, me).wait_send()
            result_copy(k, me, (me + d) % plane).wait_recv()

        result_local(k).wait()


def local(gradients, token_counts, row_groups, col_groups):
    rows, cols = lax.axis_size("row"), lax.axis_size("col")
    across = 2 if rows % 2 == 0 else 1
    depth, plane = rows // across, across * cols
    width = gradients.shape[-1]
    height = gradients.size // width // plane
    wide = 256 if width % 256 == 0 else width
    chunks = width // wide
    groups = cols
    coefficient, chosen = path_counts(row_groups, col_groups)
    pieces = gradients.reshape(plane, height, width)
    smem = pl.BlockSpec(memory_space=pltpu.SMEM)
    vmem = pl.BlockSpec(memory_space=pltpu.VMEM)
    slab = pltpu.VMEM((chunks, groups, height, wide), F32)
    sem = pltpu.SemaphoreType.DMA
    averaged, total = pl.pallas_call(
        functools.partial(kernel, (across, cols, depth, chunks, wide, groups)),
        out_shape=(
            jax.ShapeDtypeStruct((plane, height, width), F32),
            jax.ShapeDtypeStruct((1, wide), jnp.int32),
        ),
        in_specs=[smem, smem, smem, vmem],
        out_specs=(pl.BlockSpec(memory_space=pl.ANY), vmem),
        scratch_shapes=[
            pltpu.VMEM((chunks, plane, height, wide), gradients.dtype),
            slab, slab, slab, slab, slab,
            pltpu.VMEM((groups, height, wide), F32),
            pltpu.VMEM((chunks, plane, height, wide), F32),
            pltpu.VMEM((1, wide), F32),
            pltpu.VMEM((plane, 1, wide), F32),
            pltpu.VMEM((groups, 1, wide), F32),
            pltpu.VMEM((depth, groups, 1, wide), F32),
            pltpu.VMEM((groups, 1, wide), F32),
            sem((chunks, plane)), sem((chunks, plane)), sem((chunks, plane)), sem((chunks, plane)),
            sem((2, chunks)), sem((2, chunks)),
            sem((plane,)), sem((plane,)), sem((depth,)), sem((depth,)),
        ],
        compiler_params=pltpu.CompilerParams(
            collective_id=0, has_side_effects=True, vmem_limit_bytes=48 * 1024 * 1024
        ),
    )(coefficient, chosen, token_counts, pieces)
    return averaged.reshape(gradients.shape), total[:, :1]


def solution(mesh):
    placed = (P("row", "col", None, None, None), P("row", "col"), P(), P())
    return jax.shard_map(
        local,
        mesh=mesh,
        in_specs=placed,
        out_specs=(P("row", "col", None, None, None), P("row", "col")),
        check_vma=False,
    )
```

```python
import functools

import jax
import jax.numpy as jnp
from jax import lax
from jax.experimental import pallas as pl
from jax.experimental.pallas import tpu as pltpu
from jax.sharding import PartitionSpec as P

MESH = pl.DeviceIdType.MESH
F32 = jnp.float32
SKEW = 2
WIDE = 256
VMEM_GRANT = 48 * 1024 * 1024
LIMIT = 32766.0
FINE = 524200.0
SMALLEST = 1e-33


def path_counts(across, cols, z, table_ref, between_ref, second, third, paths, coef, chosen):
    hops = between_ref.shape[2]

    def into(turn, h, g):
        hits = [(table_ref[turn, g, between_ref[0, j, h]] == j).astype(jnp.int32) for j in range(cols)]
        return functools.reduce(lambda one, two: one + two, hits)

    @pl.loop(0, hops)
    def _(h):
        for g in range(cols):
            second[h, g] = into(0, h, g)
            third[h, g] = into(1, h, g)

    @pl.loop(0, cols)
    def _(k):
        for g in range(cols):
            paths[k, g] = functools.reduce(
                lambda one, two: one + two, [third[h, k] * second[h, g] for h in range(hops)])

    @pl.loop(0, across * cols)
    def _(q):
        i, j = z * across + q // cols, q % cols
        mine = last = jnp.int32(0)
        for g in range(cols):
            mine = jnp.where(table_ref[0, g, i] == j, g, mine)
            last = jnp.where(table_ref[1, g, i] == j, g, last)
        chosen[q] = last
        for k in range(cols):
            coef[q, k] = paths[k, mine]


def encode(value, k, groups, code_ref, step_ref):
    for low in range(0, groups, 4):
        packed = None
        for g in range(low, min(low + 4, groups)):
            part = value(g)
            step = jnp.maximum(jnp.max(jnp.abs(part), axis=0, keepdims=True), SMALLEST) * (1.0 / FINE)
            step_ref[k, g] = step
            code = jnp.round(part * (1.0 / step)).astype(jnp.int32)
            code_ref[k, g] = (code >> 4).astype(jnp.int16)
            bits = (code & 15) << (4 * (g - low))
            packed = bits if packed is None else packed + bits
        code_ref[k, groups + low // 4] = (packed - 32768).astype(jnp.int16)


def decode(k, groups, code_ref, step_ref, value_ref):
    for low in range(0, groups, 4):
        packed = code_ref[k, groups + low // 4].astype(jnp.int32) + 32768
        for g in range(low, min(low + 4, groups)):
            code = code_ref[k, g].astype(jnp.int32) * 16 + ((packed >> (4 * (g - low))) & 15)
            value_ref[k, g] = code.astype(F32) * step_ref[k, g]


def kernel(
    geometry,
    table_ref, between_ref, count_ref, x_hbm,
    out_ref, scale_ref, total_ref,
    x_ref, recv, own, up_sum, down_sum, up_out, up_in, down_out, down_in,
    up_out_step, up_in_step, down_out_step, down_in_step, codes, steps, ret, ret_scale,
    cnt_send, cnt, part_send, parts, inverse, factor,
    second, third, paths, coef, chosen, load_sem,
    x_send_sem, x_recv_sem, r_send_sem, r_recv_sem, s_send_sem, s_recv_sem, z_send_sem, z_recv_sem, zs_send_sem, zs_recv_sem,
    c_send_sem, c_recv_sem, p_send_sem, p_recv_sem,
):
    across, cols, depth, chunks, wide, groups = geometry
    plane = across * cols
    row, col = lax.axis_index("row"), lax.axis_index("col")
    z = row // across
    me = (row % across) * cols + col

    def member(q):
        return (z * across + q // cols, q % cols)

    def level(other):
        return (other * across + row % across, col)

    def lanes(k):
        return pl.ds(pl.multiple_of(k * wide, 128), wide)

    load = pltpu.make_async_copy(x_hbm, x_ref, load_sem)
    load.start()
    barrier = pltpu.get_barrier_semaphore()
    for d in range(1, plane):
        pl.semaphore_signal(barrier, inc=1, device_id=member((me + d) % plane), device_id_type=MESH)
    for d in range(1, depth):
        pl.semaphore_signal(barrier, inc=1, device_id=level((z + d) % depth), device_id_type=MESH)
    count = count_ref[0, 0].astype(F32)
    cnt_send[...] = jnp.full(cnt_send.shape, count, F32)
    cnt[me] = jnp.full(cnt_send.shape, count, F32)
    path_counts(across, cols, z, table_ref, between_ref, second, third, paths, coef, chosen)

    @pl.when(z == 0)
    def _():
        up_sum[...] = jnp.zeros(up_sum.shape, F32)

    @pl.when(z == depth - 1)
    def _():
        down_sum[...] = jnp.zeros(down_sum.shape, F32)

    load.wait()
    pl.semaphore_wait(barrier, plane + depth - 2)

    def count_copy(d):
        to = (me + d) % plane
        return pltpu.make_async_remote_copy(
            src_ref=cnt_send, dst_ref=cnt.at[me], send_sem=c_send_sem.at[to], recv_sem=c_recv_sem.at[me],
            device_id=member(to), device_id_type=MESH)

    def count_arrival(q):
        return pltpu.make_async_remote_copy(
            src_ref=cnt_send, dst_ref=cnt.at[q], send_sem=c_send_sem.at[q], recv_sem=c_recv_sem.at[q],
            device_id=member(q), device_id_type=MESH)

    def part_copy(d):
        to = (z + d) % depth
        return pltpu.make_async_remote_copy(
            src_ref=part_send, dst_ref=parts.at[z], send_sem=p_send_sem.at[to], recv_sem=p_recv_sem.at[z],
            device_id=level(to), device_id_type=MESH)

    def part_arrival(s):
        return pltpu.make_async_remote_copy(
            src_ref=part_send, dst_ref=parts.at[s], send_sem=p_send_sem.at[s], recv_sem=p_recv_sem.at[s],
            device_id=level(s), device_id_type=MESH)

    def piece_copy(k, to, slot):
        return pltpu.make_async_remote_copy(
            src_ref=x_ref.at[to, :, lanes(k)], dst_ref=recv.at[k, slot],
            send_sem=x_send_sem.at[k, to], recv_sem=x_recv_sem.at[k, slot],
            device_id=member(to), device_id_type=MESH)

    def result_copy(k, to, slot):
        return pltpu.make_async_remote_copy(
            src_ref=ret.at[k, to], dst_ref=out_ref.at[slot, :, lanes(k)],
            send_sem=r_send_sem.at[k, to], recv_sem=r_recv_sem.at[k, slot],
            device_id=member(to), device_id_type=MESH)

    def scale_copy(k, to, slot):
        return pltpu.make_async_remote_copy(
            src_ref=ret_scale.at[k, to], dst_ref=scale_ref.at[slot, :, lanes(k)],
            send_sem=s_send_sem.at[k, to], recv_sem=s_recv_sem.at[k, slot],
            device_id=member(to), device_id_type=MESH)

    def result_local(k):
        return pltpu.make_async_copy(ret.at[k, me], out_ref.at[me, :, lanes(k)], r_recv_sem.at[k, me])

    def scale_local(k):
        return pltpu.make_async_copy(ret_scale.at[k, me], scale_ref.at[me, :, lanes(k)], s_recv_sem.at[k, me])

    def up_step_copy(k):
        return pltpu.make_async_remote_copy(
            src_ref=up_out_step.at[k], dst_ref=up_in_step.at[k],
            send_sem=zs_send_sem.at[0, k], recv_sem=zs_recv_sem.at[0, k],
            device_id=level((z + 1) % depth), device_id_type=MESH)

    def up_copy(k):
        return pltpu.make_async_remote_copy(
            src_ref=up_out.at[k], dst_ref=up_in.at[k], send_sem=z_send_sem.at[0, k], recv_sem=z_recv_sem.at[0, k],
            device_id=level((z + 1) % depth), device_id_type=MESH)

    def down_step_copy(k):
        return pltpu.make_async_remote_copy(
            src_ref=down_out_step.at[k], dst_ref=down_in_step.at[k],
            send_sem=zs_send_sem.at[1, k], recv_sem=zs_recv_sem.at[1, k],
            device_id=level((z + depth - 1) % depth), device_id_type=MESH)

    def down_copy(k):
        return pltpu.make_async_remote_copy(
            src_ref=down_out.at[k], dst_ref=down_in.at[k], send_sem=z_send_sem.at[1, k], recv_sem=z_recv_sem.at[1, k],
            device_id=level((z + depth - 1) % depth), device_id_type=MESH)

    @pl.loop(1, plane)
    def _(d):
        count_copy(d).start()

    @pl.loop(0, chunks)
    def _(k):
        @pl.loop(1, plane)
        def _(d):
            piece_copy(k, (me + d) % plane, me).start()

    @pl.loop(1, plane)
    def _(d):
        count_arrival((me + d) % plane).wait_recv()

    for g in range(groups):
        part = None
        for q in range(plane):
            term = coef[q, g].astype(F32) * cnt[q]
            factor[q, g] = term
            part = term if q == 0 else part + term
        part_send[g] = part
        parts[z, g] = part

    @pl.loop(1, depth)
    def _(d):
        part_copy(d).start()

    far = jnp.maximum(z, depth - 1 - z)

    @pl.loop(0, chunks + SKEW * (depth - 1))
    def _(t):
        @pl.when(t < chunks)
        def _():
            recv[t, me] = x_ref[me, :, lanes(t)]

            @pl.loop(1, plane)
            def _(d):
                piece_copy(t, me, (me + d) % plane).wait_recv()

            sums = [None] * groups
            for q in range(plane):
                piece = recv[t, q].astype(F32)
                for g in range(groups):
                    term = piece * factor[q, g]
                    sums[g] = term if q == 0 else sums[g] + term
            for g in range(groups):
                own[t, g] = sums[g]

        up = t - SKEW * z

        @pl.when((up >= 0) & (up < chunks))
        def _():
            @pl.when(z > 0)
            def _():
                up_copy(up).wait_recv()
                up_step_copy(up).wait_recv()
                decode(up, groups, up_in, up_in_step, up_sum)

            @pl.when(z < depth - 1)
            def _():
                encode(lambda g: own[up, g] + up_sum[up, g], up, groups, up_out, up_out_step)
                up_step_copy(up).start()
                up_copy(up).start()

        down = t - SKEW * (depth - 1 - z)

        @pl.when((down >= 0) & (down < chunks))
        def _():
            @pl.when(z < depth - 1)
            def _():
                down_copy(down).wait_recv()
                down_step_copy(down).wait_recv()
                decode(down, groups, down_in, down_in_step, down_sum)

            @pl.when(z > 0)
            def _():
                encode(lambda g: own[down, g] + down_sum[down, g], down, groups, down_out, down_out_step)
                down_step_copy(down).start()
                down_copy(down).start()

        end = t - SKEW * far

        @pl.when(end == 0)
        def _():
            @pl.loop(1, depth)
            def _(d):
                part_arrival((z + d) % depth).wait_recv()

            for g in range(groups):
                weight = parts[0, g]
                for s in range(1, depth):
                    weight = weight + parts[s, g]
                parts[z, g] = weight
                inverse[g] = 1.0 / weight
            total_ref[...] = parts[z, chosen[me], :, :1].astype(jnp.int32)

        @pl.when((end >= 0) & (end < chunks))
        def _():
            for g in range(groups):
                mean = (own[end, g] + up_sum[end, g] + down_sum[end, g]) * inverse[g]
                step = jnp.maximum(jnp.max(jnp.abs(mean), axis=0, keepdims=True), SMALLEST) * (1.0 / LIMIT)
                steps[g] = step
                codes[g] = jnp.round(mean * (1.0 / step)).astype(jnp.int32).astype(jnp.int16)

            @pl.loop(1, plane)
            def _(d):
                to = (me + d) % plane
                ret[end, to] = codes[chosen[to]]
                ret_scale[end, to] = steps[chosen[to]]
                result_copy(end, to, me).start()
                scale_copy(end, to, me).start()

            ret[end, me] = codes[chosen[me]]
            ret_scale[end, me] = steps[chosen[me]]
            result_local(end).start()
            scale_local(end).start()

    @pl.loop(1, plane)
    def _(d):
        count_copy(d).wait_send()

    @pl.loop(1, depth)
    def _(d):
        part_copy(d).wait_send()

    @pl.loop(0, chunks)
    def _(k):
        @pl.when(z < depth - 1)
        def _():
            up_copy(k).wait_send()
            up_step_copy(k).wait_send()

        @pl.when(z > 0)
        def _():
            down_copy(k).wait_send()
            down_step_copy(k).wait_send()

        @pl.loop(1, plane)
        def _(d):
            piece_copy(k, (me + d) % plane, me).wait_send()
            result_copy(k, (me + d) % plane, me).wait_send()
            result_copy(k, me, (me + d) % plane).wait_recv()
            scale_copy(k, (me + d) % plane, me).wait_send()
            scale_copy(k, me, (me + d) % plane).wait_recv()

        result_local(k).wait()
        scale_local(k).wait()


def local(gradients, token_counts, row_groups, col_groups):
    rows, cols = lax.axis_size("row"), lax.axis_size("col")
    across = 2 if rows % 2 == 0 else 1
    depth, plane = rows // across, across * cols
    width = gradients.shape[-1]
    height = gradients.size // width // plane
    wide = WIDE if width % WIDE == 0 else width
    chunks = width // wide
    groups = cols
    pieces = gradients.reshape(plane, height, width)
    smem = pl.BlockSpec(memory_space=pltpu.SMEM)
    vmem = pl.BlockSpec(memory_space=pltpu.VMEM)
    slab = pltpu.VMEM((chunks, groups, height, wide), F32)
    coded = pltpu.VMEM((chunks, groups + pl.cdiv(groups, 4), height, wide), jnp.int16)
    step = pltpu.VMEM((chunks, groups, 1, wide), F32)
    sem = pltpu.SemaphoreType.DMA
    codes, scales, total = pl.pallas_call(
        functools.partial(kernel, (across, cols, depth, chunks, wide, groups)),
        out_shape=(
            jax.ShapeDtypeStruct((plane, height, width), jnp.int16),
            jax.ShapeDtypeStruct((plane, 1, width), F32),
            jax.ShapeDtypeStruct((1, 1), jnp.int32),
        ),
        in_specs=[smem, smem, smem, pl.BlockSpec(memory_space=pltpu.HBM)],
        out_specs=(vmem, vmem, vmem),
        scratch_shapes=[
            pltpu.VMEM((plane, height, width), gradients.dtype),
            pltpu.VMEM((chunks, plane, height, wide), gradients.dtype),
            slab, slab, slab, coded, coded, coded, coded, step, step, step, step,
            pltpu.VMEM((groups, height, wide), jnp.int16),
            pltpu.VMEM((groups, 1, wide), F32),
            pltpu.VMEM((chunks, plane, height, wide), jnp.int16),
            pltpu.VMEM((chunks, plane, 1, wide), F32),
            pltpu.VMEM((1, wide), F32),
            pltpu.VMEM((plane, 1, wide), F32),
            pltpu.VMEM((groups, 1, wide), F32),
            pltpu.VMEM((depth, groups, 1, wide), F32),
            pltpu.VMEM((groups, 1, wide), F32),
            pltpu.VMEM((plane, groups, 1, wide), F32),
            pltpu.SMEM((rows, groups), jnp.int32),
            pltpu.SMEM((rows, groups), jnp.int32),
            pltpu.SMEM((groups, groups), jnp.int32),
            pltpu.SMEM((plane, groups), jnp.int32),
            pltpu.SMEM((plane,), jnp.int32),
            sem,
            sem((chunks, plane)), sem((chunks, plane)), sem((chunks, plane)), sem((chunks, plane)),
            sem((chunks, plane)), sem((chunks, plane)),
            sem((2, chunks)), sem((2, chunks)), sem((2, chunks)), sem((2, chunks)),
            sem((plane,)), sem((plane,)), sem((depth,)), sem((depth,)),
        ],
        compiler_params=pltpu.CompilerParams(
            collective_id=0, has_side_effects=True, vmem_limit_bytes=VMEM_GRANT
        ),
    )(jnp.swapaxes(row_groups, 1, 2), col_groups, token_counts, pieces)
    averaged = codes.astype(F32) * scales
    return averaged.reshape(gradients.shape), total


def solution(mesh):
    placed = (P("row", "col", None, None, None), P("row", "col"), P(), P())
    return jax.shard_map(
        local,
        mesh=mesh,
        in_specs=placed,
        out_specs=(P("row", "col", None, None, None), P("row", "col")),
        check_vma=False,
    )
```

```python
import functools

import jax
import jax.numpy as jnp
from jax import lax
from jax.experimental import pallas as pl
from jax.experimental.pallas import tpu as pltpu
from jax.sharding import PartitionSpec as P

MESH = pl.DeviceIdType.MESH
F32 = jnp.float32
SKEW = 2
WIDE = 256
VMEM_GRANT = 48 * 1024 * 1024
LIMIT = 32766.0
FINE = 524200.0
SMALLEST = 1e-33


def path_counts(across, cols, z, table_ref, between_ref, second, third, paths, coef, chosen):
    hops = between_ref.shape[2]

    def into(turn, h, g):
        hits = [(table_ref[turn, g, between_ref[0, j, h]] == j).astype(jnp.int32) for j in range(cols)]
        return functools.reduce(lambda one, two: one + two, hits)

    @pl.loop(0, hops)
    def _(h):
        for g in range(cols):
            second[h, g] = into(0, h, g)
            third[h, g] = into(1, h, g)

    @pl.loop(0, cols)
    def _(k):
        for g in range(cols):
            paths[k, g] = functools.reduce(
                lambda one, two: one + two, [third[h, k] * second[h, g] for h in range(hops)])

    @pl.loop(0, across * cols)
    def _(q):
        i, j = z * across + q // cols, q % cols
        mine = last = jnp.int32(0)
        for g in range(cols):
            mine = jnp.where(table_ref[0, g, i] == j, g, mine)
            last = jnp.where(table_ref[1, g, i] == j, g, last)
        chosen[q] = last
        for k in range(cols):
            coef[q, k] = paths[k, mine]


def encode(value, k, groups, code_ref, step_ref):
    for low in range(0, groups, 4):
        packed = None
        for g in range(low, min(low + 4, groups)):
            part = value(g)
            step = jnp.maximum(jnp.max(jnp.abs(part), axis=0, keepdims=True), SMALLEST) * (1.0 / FINE)
            step_ref[k, g] = step
            code = jnp.round(part * (1.0 / step)).astype(jnp.int32)
            code_ref[k, g] = (code >> 4).astype(jnp.int16)
            bits = (code & 15) << (4 * (g - low))
            packed = bits if packed is None else packed + bits
        code_ref[k, groups + low // 4] = (packed - 32768).astype(jnp.int16)


def decode(k, groups, code_ref, step_ref, value_ref):
    for low in range(0, groups, 4):
        packed = code_ref[k, groups + low // 4].astype(jnp.int32) + 32768
        for g in range(low, min(low + 4, groups)):
            code = code_ref[k, g].astype(jnp.int32) * 16 + ((packed >> (4 * (g - low))) & 15)
            value_ref[k, g] = code.astype(F32) * step_ref[k, g]


def kernel(
    geometry,
    table_ref, between_ref, count_ref, x_ref,
    out_ref, scale_ref, total_ref,
    recv, own, up_sum, down_sum, up_out, up_in, down_out, down_in,
    up_out_step, up_in_step, down_out_step, down_in_step, codes, steps, ret, ret_scale,
    cnt_send, cnt, part_send, parts, inverse, factor,
    second, third, paths, coef, chosen,
    x_send_sem, x_recv_sem, r_send_sem, r_recv_sem, s_send_sem, s_recv_sem, z_send_sem, z_recv_sem, zs_send_sem, zs_recv_sem,
    c_send_sem, c_recv_sem, p_send_sem, p_recv_sem,
):
    across, cols, depth, chunks, wide, groups = geometry
    plane = across * cols
    row, col = lax.axis_index("row"), lax.axis_index("col")
    z = row // across
    me = (row % across) * cols + col

    def member(q):
        return (z * across + q // cols, q % cols)

    def level(other):
        return (other * across + row % across, col)

    def lanes(k):
        return pl.ds(pl.multiple_of(k * wide, 128), wide)

    barrier = pltpu.get_barrier_semaphore()
    for d in range(1, plane):
        pl.semaphore_signal(barrier, inc=1, device_id=member((me + d) % plane), device_id_type=MESH)
    for d in range(1, depth):
        pl.semaphore_signal(barrier, inc=1, device_id=level((z + d) % depth), device_id_type=MESH)
    count = count_ref[0, 0].astype(F32)
    cnt_send[...] = jnp.full(cnt_send.shape, count, F32)
    cnt[me] = jnp.full(cnt_send.shape, count, F32)
    path_counts(across, cols, z, table_ref, between_ref, second, third, paths, coef, chosen)

    @pl.when(z == 0)
    def _():
        up_sum[...] = jnp.zeros(up_sum.shape, F32)

    @pl.when(z == depth - 1)
    def _():
        down_sum[...] = jnp.zeros(down_sum.shape, F32)

    pl.semaphore_wait(barrier, plane + depth - 2)

    def count_copy(d):
        to = (me + d) % plane
        return pltpu.make_async_remote_copy(
            src_ref=cnt_send, dst_ref=cnt.at[me], send_sem=c_send_sem.at[to], recv_sem=c_recv_sem.at[me],
            device_id=member(to), device_id_type=MESH)

    def count_arrival(q):
        return pltpu.make_async_remote_copy(
            src_ref=cnt_send, dst_ref=cnt.at[q], send_sem=c_send_sem.at[q], recv_sem=c_recv_sem.at[q],
            device_id=member(q), device_id_type=MESH)

    def part_copy(d):
        to = (z + d) % depth
        return pltpu.make_async_remote_copy(
            src_ref=part_send, dst_ref=parts.at[z], send_sem=p_send_sem.at[to], recv_sem=p_recv_sem.at[z],
            device_id=level(to), device_id_type=MESH)

    def part_arrival(s):
        return pltpu.make_async_remote_copy(
            src_ref=part_send, dst_ref=parts.at[s], send_sem=p_send_sem.at[s], recv_sem=p_recv_sem.at[s],
            device_id=level(s), device_id_type=MESH)

    def piece_copy(k, to, slot):
        return pltpu.make_async_remote_copy(
            src_ref=x_ref.at[to, :, lanes(k)], dst_ref=recv.at[k, slot],
            send_sem=x_send_sem.at[k, to], recv_sem=x_recv_sem.at[k, slot],
            device_id=member(to), device_id_type=MESH)

    def result_copy(k, to, slot):
        return pltpu.make_async_remote_copy(
            src_ref=ret.at[k, to], dst_ref=out_ref.at[slot, :, lanes(k)],
            send_sem=r_send_sem.at[k, to], recv_sem=r_recv_sem.at[k, slot],
            device_id=member(to), device_id_type=MESH)

    def scale_copy(k, to, slot):
        return pltpu.make_async_remote_copy(
            src_ref=ret_scale.at[k, to], dst_ref=scale_ref.at[slot, :, lanes(k)],
            send_sem=s_send_sem.at[k, to], recv_sem=s_recv_sem.at[k, slot],
            device_id=member(to), device_id_type=MESH)

    def result_local(k):
        return pltpu.make_async_copy(ret.at[k, me], out_ref.at[me, :, lanes(k)], r_recv_sem.at[k, me])

    def scale_local(k):
        return pltpu.make_async_copy(ret_scale.at[k, me], scale_ref.at[me, :, lanes(k)], s_recv_sem.at[k, me])

    def up_step_copy(k):
        return pltpu.make_async_remote_copy(
            src_ref=up_out_step.at[k], dst_ref=up_in_step.at[k],
            send_sem=zs_send_sem.at[0, k], recv_sem=zs_recv_sem.at[0, k],
            device_id=level((z + 1) % depth), device_id_type=MESH)

    def up_copy(k):
        return pltpu.make_async_remote_copy(
            src_ref=up_out.at[k], dst_ref=up_in.at[k], send_sem=z_send_sem.at[0, k], recv_sem=z_recv_sem.at[0, k],
            device_id=level((z + 1) % depth), device_id_type=MESH)

    def down_step_copy(k):
        return pltpu.make_async_remote_copy(
            src_ref=down_out_step.at[k], dst_ref=down_in_step.at[k],
            send_sem=zs_send_sem.at[1, k], recv_sem=zs_recv_sem.at[1, k],
            device_id=level((z + depth - 1) % depth), device_id_type=MESH)

    def down_copy(k):
        return pltpu.make_async_remote_copy(
            src_ref=down_out.at[k], dst_ref=down_in.at[k], send_sem=z_send_sem.at[1, k], recv_sem=z_recv_sem.at[1, k],
            device_id=level((z + depth - 1) % depth), device_id_type=MESH)

    @pl.loop(1, plane)
    def _(d):
        count_copy(d).start()

    @pl.loop(0, chunks)
    def _(k):
        @pl.loop(1, plane)
        def _(d):
            piece_copy(k, (me + d) % plane, me).start()

    @pl.loop(1, plane)
    def _(d):
        count_arrival((me + d) % plane).wait_recv()

    for g in range(groups):
        part = None
        for q in range(plane):
            term = coef[q, g].astype(F32) * cnt[q]
            factor[q, g] = term
            part = term if q == 0 else part + term
        part_send[g] = part
        parts[z, g] = part

    @pl.loop(1, depth)
    def _(d):
        part_copy(d).start()

    far = jnp.maximum(z, depth - 1 - z)

    @pl.loop(0, chunks + SKEW * (depth - 1))
    def _(t):
        @pl.when(t < chunks)
        def _():
            recv[t, me] = x_ref[me, :, lanes(t)]

            @pl.loop(1, plane)
            def _(d):
                piece_copy(t, me, (me + d) % plane).wait_recv()

            sums = [None] * groups
            for q in range(plane):
                piece = recv[t, q].astype(F32)
                for g in range(groups):
                    term = piece * factor[q, g]
                    sums[g] = term if q == 0 else sums[g] + term
            for g in range(groups):
                own[t, g] = sums[g]

        up = t - SKEW * z

        @pl.when((up >= 0) & (up < chunks))
        def _():
            @pl.when(z > 0)
            def _():
                up_copy(up).wait_recv()
                up_step_copy(up).wait_recv()
                decode(up, groups, up_in, up_in_step, up_sum)

            @pl.when(z < depth - 1)
            def _():
                encode(lambda g: own[up, g] + up_sum[up, g], up, groups, up_out, up_out_step)
                up_step_copy(up).start()
                up_copy(up).start()

        down = t - SKEW * (depth - 1 - z)

        @pl.when((down >= 0) & (down < chunks))
        def _():
            @pl.when(z < depth - 1)
            def _():
                down_copy(down).wait_recv()
                down_step_copy(down).wait_recv()
                decode(down, groups, down_in, down_in_step, down_sum)

            @pl.when(z > 0)
            def _():
                encode(lambda g: own[down, g] + down_sum[down, g], down, groups, down_out, down_out_step)
                down_step_copy(down).start()
                down_copy(down).start()

        end = t - SKEW * far

        @pl.when(end == 0)
        def _():
            @pl.loop(1, depth)
            def _(d):
                part_arrival((z + d) % depth).wait_recv()

            for g in range(groups):
                weight = parts[0, g]
                for s in range(1, depth):
                    weight = weight + parts[s, g]
                parts[z, g] = weight
                inverse[g] = 1.0 / weight
            total_ref[...] = parts[z, chosen[me], :, :1].astype(jnp.int32)

        @pl.when((end >= 0) & (end < chunks))
        def _():
            for g in range(groups):
                mean = (own[end, g] + up_sum[end, g] + down_sum[end, g]) * inverse[g]
                step = jnp.maximum(jnp.max(jnp.abs(mean), axis=0, keepdims=True), SMALLEST) * (1.0 / LIMIT)
                steps[g] = step
                codes[g] = jnp.round(mean * (1.0 / step)).astype(jnp.int32).astype(jnp.int16)

            @pl.loop(1, plane, unroll=True)
            def _(d):
                to = (me + d) % plane
                ret[end, to] = codes[chosen[to]]
                ret_scale[end, to] = steps[chosen[to]]
                result_copy(end, to, me).start()
                scale_copy(end, to, me).start()

            ret[end, me] = codes[chosen[me]]
            ret_scale[end, me] = steps[chosen[me]]
            result_local(end).start()
            scale_local(end).start()

    @pl.loop(1, plane)
    def _(d):
        count_copy(d).wait_send()

    @pl.loop(1, depth)
    def _(d):
        part_copy(d).wait_send()

    @pl.loop(0, chunks)
    def _(k):
        @pl.when(z < depth - 1)
        def _():
            up_copy(k).wait_send()
            up_step_copy(k).wait_send()

        @pl.when(z > 0)
        def _():
            down_copy(k).wait_send()
            down_step_copy(k).wait_send()

        @pl.loop(1, plane)
        def _(d):
            piece_copy(k, (me + d) % plane, me).wait_send()
            result_copy(k, (me + d) % plane, me).wait_send()
            result_copy(k, me, (me + d) % plane).wait_recv()
            scale_copy(k, (me + d) % plane, me).wait_send()
            scale_copy(k, me, (me + d) % plane).wait_recv()

        result_local(k).wait()
        scale_local(k).wait()


def local(gradients, token_counts, row_groups, col_groups):
    rows, cols = lax.axis_size("row"), lax.axis_size("col")
    across = 2 if rows % 2 == 0 else 1
    depth, plane = rows // across, across * cols
    width = gradients.shape[-1]
    height = gradients.size // width // plane
    wide = WIDE if width % WIDE == 0 else width
    chunks = width // wide
    groups = cols
    pieces = gradients.reshape(plane, height, width)
    smem = pl.BlockSpec(memory_space=pltpu.SMEM)
    vmem = pl.BlockSpec(memory_space=pltpu.VMEM)
    slab = pltpu.VMEM((chunks, groups, height, wide), F32)
    coded = pltpu.VMEM((chunks, groups + pl.cdiv(groups, 4), height, wide), jnp.int16)
    step = pltpu.VMEM((chunks, groups, 1, wide), F32)
    sem = pltpu.SemaphoreType.DMA
    codes, scales, total = pl.pallas_call(
        functools.partial(kernel, (across, cols, depth, chunks, wide, groups)),
        out_shape=(
            jax.ShapeDtypeStruct((plane, height, width), jnp.int16),
            jax.ShapeDtypeStruct((plane, 1, width), F32),
            jax.ShapeDtypeStruct((1, 1), jnp.int32),
        ),
        in_specs=[smem, smem, smem, vmem],
        out_specs=(vmem, vmem, vmem),
        scratch_shapes=[
            pltpu.VMEM((chunks, plane, height, wide), gradients.dtype),
            slab, slab, slab, coded, coded, coded, coded, step, step, step, step,
            pltpu.VMEM((groups, height, wide), jnp.int16),
            pltpu.VMEM((groups, 1, wide), F32),
            pltpu.VMEM((chunks, plane, height, wide), jnp.int16),
            pltpu.VMEM((chunks, plane, 1, wide), F32),
            pltpu.VMEM((1, wide), F32),
            pltpu.VMEM((plane, 1, wide), F32),
            pltpu.VMEM((groups, 1, wide), F32),
            pltpu.VMEM((depth, groups, 1, wide), F32),
            pltpu.VMEM((groups, 1, wide), F32),
            pltpu.VMEM((plane, groups, 1, wide), F32),
            pltpu.SMEM((rows, groups), jnp.int32),
            pltpu.SMEM((rows, groups), jnp.int32),
            pltpu.SMEM((groups, groups), jnp.int32),
            pltpu.SMEM((plane, groups), jnp.int32),
            pltpu.SMEM((plane,), jnp.int32),
            sem((chunks, plane)), sem((chunks, plane)), sem((chunks, plane)), sem((chunks, plane)),
            sem((chunks, plane)), sem((chunks, plane)),
            sem((2, chunks)), sem((2, chunks)), sem((2, chunks)), sem((2, chunks)),
            sem((plane,)), sem((plane,)), sem((depth,)), sem((depth,)),
        ],
        compiler_params=pltpu.CompilerParams(
            collective_id=0, has_side_effects=True, vmem_limit_bytes=VMEM_GRANT
        ),
    )(jnp.swapaxes(row_groups, 1, 2), col_groups, token_counts, pieces)
    averaged = codes.astype(F32) * scales
    return averaged.reshape(gradients.shape), total


def solution(mesh):
    placed = (P("row", "col", None, None, None), P("row", "col"), P(), P())
    return jax.shard_map(
        local,
        mesh=mesh,
        in_specs=placed,
        out_specs=(P("row", "col", None, None, None), P("row", "col")),
        check_vma=False,
    )
```
